256 devices in a mesh: row: 16 (over x_hi, z), col: 8 (over x_lo, y), rep: 2 (over core).
Axes of the slice: x: 4 (x_hi: 2, x_lo: 2; x = x_hi * 2 + x_lo), y: 4, z: 8, core: 2. Of those that a mesh axis runs over, the one named last changes fastest.
Arguments:
- matrix: float32 [16384, 16384], P('row', 'col'), may hold values from -0.125 to 0.125
- vectors: float32 [64, 16384], P('rep', 'row'), may hold values from -0.3 to 0.3
Outputs:
- result: float32 [64, 16384], P('rep', 'row')
The draws below stay inside these ranges and needn't reach their ends.
All inputs are finite; a program needn't handle non-finite values.
Results may differ from the reference program's by a relative error of at most 0.00011.
Values sent between devices are 32-bit elements; how exact they have to be, the bound alone decides.
A program may use at most 64 MiB of HBM per device.

```python
import jax
import jax.numpy as jnp
from jax import lax

N = 16384
COLS = 64
TERMS = 6
STEPS = 1


def block_scale(rng, dims, split, smallest, largest):
    factor_of = 1.0
    for position, blocks in split:
        steps = jax.random.uniform(jax.random.fold_in(jax.random.fold_in(rng, 6), position), (blocks,), jnp.float32, smallest / len(split), largest / len(split))
        factor_of = factor_of * jnp.repeat(jnp.exp(steps), dims[position] // blocks).reshape((-1,) + (1,) * (len(dims) - 1 - position))
    return factor_of


def gaussian(stream_key, shape, deviation, limit, pieces=(), dtype=jnp.bfloat16):
    factor_of = block_scale(stream_key, shape, pieces, -0.22, 0.18) if pieces else 1.0
    entries = jax.random.normal(stream_key, shape, jnp.float32) * deviation * factor_of
    return jnp.minimum(jnp.maximum(entries, -limit), limit).astype(dtype)


def setup_inputs(seed: int = 0) -> dict:
    key_list = jax.random.split(jax.random.key(seed), 3)
    matrix = gaussian(key_list[0], (N, N), (N // 7) ** -0.5, 0.125, ((0, 16), (1, 8)), jnp.float32)
    vectors = gaussian(key_list[1], (COLS, N), 0.05, 0.3, ((0, 2), (1, 16)), jnp.float32)
    return {"matrix": matrix, "vectors": vectors}


def reference(matrix, vectors):
    current = vectors
    for section in range(STEPS):
        summand = current
        running = current
        for degree in range(1, TERMS + 1):
            product = lax.dot_general(summand, matrix, (((1,), (1,)), ((), ())), precision=lax.Precision.HIGHEST, preferred_element_type=jnp.float32)
            summand = product / float(degree * STEPS)
            running = running + summand
        current = running
    return current
```

```python
import functools

import jax
import jax.numpy as jnp
from jax import lax
from jax.experimental import pallas as pl
from jax.experimental.pallas import tpu as pltpu
from jax.sharding import PartitionSpec as P

TERMS = 6
STEPS = 1
CHUNKS = 2
ROWS = 32 // CHUNKS
PIECE = 256
PIECES = 8
MESH = pl.DeviceIdType.MESH


def kernel(
    matrix_hbm,
    vectors_hbm,
    result_ref,
    stage,
    w_high,
    w_low,
    vectors_ref,
    start_piece,
    operand,
    partial_out,
    partial_in,
    summand,
    total,
    total_in,
    stage_sem,
    vectors_sem,
    piece_sem,
    operand_sem,
    partial_sem,
    total_sem,
    operand_send,
    partial_send,
    total_send,
):
    row, col, rep = lax.axis_index("row"), lax.axis_index("col"), lax.axis_index("rep")
    z, y = row % 8, col % 4
    x = (row // 8) * 2 + col // 4
    outer = (x == 0) | (x == 3)
    swapped = jnp.where(outer, x, 3 - x)
    parity = z % 2

    def device(dx, dy, dz):
        return ((dx // 2) * 8 + dz, (dx % 2) * 4 + dy, rep)

    def remote(dx, dy, dz):
        return (dx != x) | (dy != y) | (dz != z)

    partial_to = [
        (x // 2 + 2 * half, (y + step) % 4, z) for step in (2, 1, 3, 0) for half in (0, 1)
    ]
    partial_from = [(2 * (x % 2) + low, other, z) for other in range(4) for low in (0, 1)]
    operand_to = [(z // 2, (z + step) % 8) for step in (4, 3, 5, 2, 6, 1, 7, 0)]
    operand_from = [(other, 2 * y + which) for other in range(4) for which in (0, 1)]
    total_to = [(swapped, (y + step) % 4, z) for step in (2, 1, 3, 0)]

    def stage_copy(piece):
        return pltpu.make_async_copy(
            matrix_hbm.at[:, pl.ds(piece * PIECE, PIECE)], stage.at[piece], stage_sem.at[piece]
        )

    def piece_copy(chunk):
        return pltpu.make_async_copy(
            vectors_hbm.at[pl.ds(chunk * ROWS, ROWS), pl.ds(pl.multiple_of(y * PIECE, PIECE), PIECE)],
            start_piece.at[chunk],
            piece_sem.at[chunk],
        )

    vectors_copy = pltpu.make_async_copy(vectors_hbm, vectors_ref, vectors_sem)
    for chunk in range(CHUNKS):
        piece_copy(chunk).start()
    for piece in range(PIECES):
        stage_copy(piece).start()
    vectors_copy.start()

    barrier = pltpu.get_barrier_semaphore()
    greeted = partial_to + partial_from + total_to
    greeted += [(x, *rest) for rest in operand_to + operand_from]
    greeted += [(swapped, *rest) for rest in operand_to + operand_from]
    count = 0
    for place in greeted:
        there = remote(*place)

        @pl.when(there)
        def _():
            pl.semaphore_signal(barrier, inc=1, device_id=device(*place), device_id_type=MESH)

        count = count + there.astype(jnp.int32)
    pl.semaphore_wait(barrier, count)

    def send(source, target, send_sem, recv_sem, place):
        @pl.when(remote(*place))
        def _():
            pltpu.make_async_remote_copy(
                src_ref=source,
                dst_ref=target,
                send_sem=send_sem,
                recv_sem=recv_sem,
                device_id=device(*place),
                device_id_type=MESH,
            ).start()

    def send_operand(source, across, degree, chunk):
        slot = parity * 4 + y
        for rest in operand_to:
            send(
                source,
                operand.at[degree, chunk, slot],
                operand_send.at[degree, chunk],
                operand_sem.at[degree, chunk, slot],
                (across, *rest),
            )

    for chunk in range(CHUNKS):
        piece_copy(chunk).wait()
        send_operand(start_piece.at[chunk], swapped, 0, chunk)

        @pl.when(outer & (z // 2 == y))
        def _():
            operand[0, chunk, parity * 4 + y] = start_piece[chunk]

    for piece in range(PIECES):
        stage_copy(piece).wait()

        def split(block, _):
            at = pl.ds(pl.multiple_of(block * PIECE, PIECE), PIECE)
            turned = stage[piece, at, :].T
            high = turned.astype(jnp.bfloat16)
            w_high[piece, :, at] = high
            w_low[piece, :, at] = (turned - high.astype(jnp.float32)).astype(jnp.bfloat16)
            return 0

        lax.fori_loop(0, 1024 // PIECE, split, 0)

    total[...] = jnp.zeros_like(total)

    def multiply(degree, chunk):
        acc = jnp.zeros((ROWS, 1024), jnp.float32)
        for step in (0, 1, 3, 2):
            for which in (0, 1):
                other = (y + step) % 4
                slot = which * 4 + other
                arrival = pltpu.make_async_copy(
                    operand.at[degree - 1, chunk, slot],
                    operand.at[degree - 1, chunk, slot],
                    operand_sem.at[degree - 1, chunk, slot],
                )
                if step == 0:
                    own = (2 * y + which == z) & (outer | (degree > 1))
                    pl.when(jnp.logical_not(own))(arrival.wait)
                else:
                    arrival.wait()
                value = operand[degree - 1, chunk, slot]
                high = value.astype(jnp.bfloat16)
                low = (value - high.astype(jnp.float32)).astype(jnp.bfloat16)
                both = jnp.dot(
                    jnp.concatenate([high, low], axis=0),
                    w_high[slot],
                    preferred_element_type=jnp.float32,
                )
                small = jnp.dot(high, w_low[slot], preferred_element_type=jnp.float32)
                acc = acc + (both[:ROWS] + (both[ROWS:] + small))
        for piece in range(4):
            partial_out[degree - 1, chunk, piece] = acc[:, piece * PIECE : (piece + 1) * PIECE]
        slot = (x % 2) * 4 + y

        @pl.when(outer)
        def _():
            partial_in[degree - 1, chunk, slot] = partial_out[degree - 1, chunk, y]

        for place in partial_to:
            send(
                partial_out.at[degree - 1, chunk, place[1]],
                partial_in.at[degree - 1, chunk, slot],
                partial_send.at[degree - 1, chunk],
                partial_sem.at[degree - 1, chunk, slot],
                place,
            )

    def add_up(degree, chunk, scale):
        for low in (0, 1):
            for other in range(4):
                slot = low * 4 + other
                own = outer & (other == y) & (x % 2 == low)
                arrival = pltpu.make_async_copy(
                    partial_in.at[degree - 1, chunk, slot],
                    partial_in.at[degree - 1, chunk, slot],
                    partial_sem.at[degree - 1, chunk, slot],
                )
                pl.when(jnp.logical_not(own))(arrival.wait)
        value = partial_in[degree - 1, chunk, 0]
        for slot in range(1, PIECES):
            value = value + partial_in[degree - 1, chunk, slot]
        return value * scale

    def section(degree, _):
        scale = jnp.float32(1.0 / STEPS)
        for which in range(2, TERMS):
            scale = jnp.where(degree == which, jnp.float32(1.0 / (which * STEPS)), scale)
        for chunk in range(CHUNKS):
            multiply(degree, chunk)
        for chunk in range(CHUNKS):
            value = add_up(degree, chunk, scale)
            summand[degree, chunk] = value
            send_operand(summand.at[degree, chunk], x, degree, chunk)

            @pl.when(z // 2 == y)
            def _():
                operand[degree, chunk, parity * 4 + y] = value

            total[chunk] += value
        return 0

    lax.fori_loop(1, TERMS, section, 0)
    for chunk in range(CHUNKS):
        multiply(TERMS, chunk)
    vectors_copy.wait()
    for chunk in range(CHUNKS):
        total[chunk] += add_up(TERMS, chunk, jnp.float32(1.0 / (TERMS * STEPS)))

        @pl.when(outer)
        def _():
            total_in[chunk, y] = total[chunk]

        for place in total_to:
            send(
                total.at[chunk],
                total_in.at[chunk, y],
                total_send.at[chunk],
                total_sem.at[chunk, y],
                place,
            )
    for chunk in range(CHUNKS):
        at = pl.ds(chunk * ROWS, ROWS)
        for other in range(4):
            arrival = pltpu.make_async_copy(
                total_in.at[chunk, other], total_in.at[chunk, other], total_sem.at[chunk, other]
            )
            pl.when(jnp.logical_not(outer & (other == y)))(arrival.wait)
            columns = pl.ds(other * PIECE, PIECE)
            result_ref[at, columns] = vectors_ref[at, columns] + total_in[chunk, other]

    def sent(sem, buffer, all_but_one):
        def wait(number):
            part = buffer.at[pl.ds(0, number)]
            pltpu.make_async_copy(part, part, sem).wait()

        full = buffer.shape[0]
        pl.when(all_but_one)(lambda: wait(full - 1))
        pl.when(jnp.logical_not(all_but_one))(lambda: wait(full))

    at_home = z // 2 == y

    def finish(degree, _):
        for chunk in range(CHUNKS):
            sent(operand_send.at[degree, chunk], operand.at[degree, chunk], at_home & (outer | (degree > 0)))
            sent(partial_send.at[degree, chunk], partial_in.at[degree, chunk], outer)
        return 0

    lax.fori_loop(0, TERMS, finish, 0)
    for chunk in range(CHUNKS):
        sent(total_send.at[chunk], total_in.at[chunk], outer)


def local(matrix, vectors):
    dma = pltpu.SemaphoreType.DMA
    float32, bfloat16 = jnp.float32, jnp.bfloat16
    return pl.pallas_call(
        kernel,
        out_shape=jax.ShapeDtypeStruct(vectors.shape, float32),
        in_specs=[pl.BlockSpec(memory_space=pl.ANY)] * 2,
        out_specs=pl.BlockSpec(memory_space=pltpu.VMEM),
        scratch_shapes=[
            pltpu.VMEM((PIECES, 1024, PIECE), float32),
            pltpu.VMEM((PIECES, PIECE, 1024), bfloat16),
            pltpu.VMEM((PIECES, PIECE, 1024), bfloat16),
            pltpu.VMEM((32, 1024), float32),
            pltpu.VMEM((CHUNKS, ROWS, PIECE), float32),
            pltpu.VMEM((TERMS, CHUNKS, PIECES, ROWS, PIECE), float32),
            pltpu.VMEM((TERMS, CHUNKS, 4, ROWS, PIECE), float32),
            pltpu.VMEM((TERMS, CHUNKS, PIECES, ROWS, PIECE), float32),
            pltpu.VMEM((TERMS, CHUNKS, ROWS, PIECE), float32),
            pltpu.VMEM((CHUNKS, ROWS, PIECE), float32),
            pltpu.VMEM((CHUNKS, 4, ROWS, PIECE), float32),
            dma((PIECES,)),
            dma,
            dma((CHUNKS,)),
            dma((TERMS, CHUNKS, PIECES)),
            dma((TERMS, CHUNKS, PIECES)),
            dma((CHUNKS, 4)),
            dma((TERMS, CHUNKS)),
            dma((TERMS, CHUNKS)),
            dma((CHUNKS,)),
        ],
        compiler_params=pltpu.CompilerParams(
            collective_id=0, has_side_effects=True, vmem_limit_bytes=48 * 2**20
        ),
    )(matrix, vectors)


def solution(mesh):
    return jax.shard_map(
        local,
        mesh=mesh,
        in_specs=(P("row", "col"), P("rep", "row")),
        out_specs=P("rep", "row"),
        check_vma=False,
    )
```
